512 devices in a mesh: pipe: 2 (over core), tensor: 8 (over x, y_hi), expert: 32 (over y_lo, z).
Axes of the slice: x: 4, y: 8 (y_hi: 2, y_lo: 4; y = y_hi * 4 + y_lo), z: 8, core: 2. Of those that a mesh axis runs over, the one named last changes fastest.
Arguments:
- tokens: bfloat16 [3, 1536, 4096], P(None, 'expert', 'tensor'), may hold values from -36 to 36
- norm_gain: float32 [2, 4096], P('pipe'), may hold values from 0.1 to 1.9
- shared_gate: bfloat16 [2, 4096, 1024], P('pipe', 'expert', 'tensor'), may hold values from -0.09375 to 0.09375
- shared_up: bfloat16 [2, 4096, 1024], P('pipe', 'expert', 'tensor'), may hold values from -0.09375 to 0.09375
- shared_down: bfloat16 [2, 1024, 4096], P('pipe', 'tensor', 'expert'), may hold values from -0.1875 to 0.1875
- expert_gate: bfloat16 [2, 32, 4096, 1024], P('pipe', 'expert', None, 'tensor'), may hold values from -0.09375 to 0.09375
- expert_up: bfloat16 [2, 32, 4096, 1024], P('pipe', 'expert', None, 'tensor'), may hold values from -0.09375 to 0.09375
- expert_down: bfloat16 [2, 32, 1024, 4096], P('pipe', 'expert', 'tensor'), may hold values from -0.1875 to 0.1875
- expert_ids: int32 [2, 3, 1536, 8], P('pipe', None, 'expert'), may hold values from 0 to 255, as said below
- expert_slots: int32 [2, 3, 1536, 8], P('pipe', None, 'expert'), may hold values from -1 to 2, as said below
- route_weights: float32 [2, 3, 1536, 8], P('pipe', None, 'expert'), may hold values from 0.1 to 1
Outputs:
- states: bfloat16 [2, 3, 1536, 4096], P('pipe', None, 'expert', 'tensor')
The draws below stay inside these ranges and needn't reach their ends.
Inputs may be any that keep to these rules, and one draw needn't show every extreme that they name: `expert_ids`: the 8 ids of a token are distinct. Ids of 32 and above name experts that are not held and add nothing. `expert_slots`: for a choice whose id is below 32: the number of earlier choices (earlier tokens, or lower k of the same token) of the same block of 48 tokens, same layer and microbatch, that name the same expert, if that number is below 3; otherwise -1. For ids of 32 and above: -1.
All inputs are finite; a program needn't handle non-finite values.
Results may differ from the reference program's by a relative error of at most 0.0085.
Values may be sent and summed in bfloat16 or wider, within the bound.
No kernel may reach another device: no remote copies, remote signals or barrier semaphores. Data moves between devices by JAX's collectives and lax.ppermute only.
A program may use at most 64 MiB of HBM per device.

```python
import math
import jax
import jax.numpy as jnp
from jax import lax

D = 4096
FE = 1024
FS = 1024
ROUTED = 256
TOP = 8
CAP = 3
TE = 48
MB = 3
LAYERS = 2
HELD = 32
FE_DEV = 128
TOKENS = 1536
N_TENSOR = 8


def route_table(key):
    subkeys = jax.random.split(jax.random.fold_in(key, 7001), 4)
    blocks = TOKENS // TE
    jitter = jax.random.randint(subkeys[0], (LAYERS, MB, TOKENS, ROUTED), 0, 2 ** 20, dtype=jnp.int32)
    popular = jax.random.randint(subkeys[1], (LAYERS, MB, 1, ROUTED), 0, 2, dtype=jnp.int32) * 2 ** 17
    hot_expert = jax.random.randint(subkeys[2], (LAYERS, MB, 1, 1), 0, HELD, dtype=jnp.int32)
    shuffle = jax.random.randint(subkeys[3], (LAYERS, MB, blocks, TE), 0, 2 ** 30, dtype=jnp.int32)
    position = jnp.argsort(jnp.argsort(shuffle, axis=-1, stable=True), axis=-1, stable=True)
    forced = (position < CAP + 1).reshape(LAYERS, MB, TOKENS, 1)
    column = jnp.arange(ROUTED, dtype=jnp.int32)
    lifted = jnp.where(forced & (column == hot_expert), 2 ** 21, 0).astype(jnp.int32)
    scores = (jitter + popular + lifted) * ROUTED + column
    chosen = lax.top_k(scores, TOP)[1].astype(jnp.int32)
    flat = chosen.reshape(LAYERS, MB, blocks, TE * TOP)
    in_window = flat < HELD
    matches = ((flat[..., None] == jnp.arange(HELD, dtype=jnp.int32)) & in_window[..., None]).astype(jnp.int32)
    earlier = jnp.cumsum(matches, axis=-2) - matches
    counted = jnp.sum(earlier * matches, axis=-1)
    slot_rank = jnp.where(in_window & (counted < CAP), counted, -1).astype(jnp.int32)
    return (chosen, slot_rank.reshape(LAYERS, MB, TOKENS, TOP))


def draw_expert_ids(key, part):
    return route_table(key)[0]


def draw_expert_slots(key, part):
    return route_table(key)[1]


def draw_tokens(key, part):
    subkeys = jax.random.split(jax.random.fold_in(key, 31), 3)
    row_scale = jnp.exp(jax.random.uniform(subkeys[0], (MB, TOKENS, 1), jnp.float32, jnp.log(0.3), jnp.log(3.0)))
    column_scale = jnp.exp(jax.random.uniform(subkeys[1], (1, 1, D), jnp.float32, jnp.log(0.3), jnp.log(3.0)))
    entries = jnp.clip(jax.random.normal(subkeys[2], (MB, TOKENS, D), jnp.float32), -4.0, 4.0)
    return jnp.clip(entries * row_scale * column_scale, -36.0, 36.0).astype(jnp.bfloat16)


def steps_of(rng, shape, cuts, smallest, top_value):
    loudness, own = 1.0, jax.random.fold_in(rng, 6)
    for axis_at, blocks in cuts:
        heights = jnp.exp(jax.random.uniform(jax.random.fold_in(own, axis_at), (blocks,), jnp.float32, smallest / len(cuts), top_value / len(cuts)))
        loudness = loudness * jnp.repeat(heights, shape[axis_at] // blocks).reshape([-1 if axis == axis_at else 1 for axis in range(len(shape))])
    return loudness


def bell_draw(own_key, extent, spread, most, cuts=(), held_as=jnp.bfloat16):
    loudness = steps_of(own_key, extent, cuts, -0.22, 0.18) if cuts else 1.0
    array = jax.random.normal(own_key, extent, jnp.float32) * spread * loudness
    return jnp.minimum(jnp.maximum(array, -most), most).astype(held_as)


def setup_inputs(seed: int = 0) -> dict:
    key_of = jax.random.split(jax.random.key(seed), 12)
    return {
        "tokens": draw_tokens(jax.random.fold_in(key_of[11], 71), 0),
        "norm_gain": jnp.clip(1.0 + 0.18 * jax.random.normal(key_of[1], (LAYERS, D), jnp.float32), 0.1, 1.9),
        "shared_gate": bell_draw(key_of[2], (LAYERS, D, FS), D ** -0.5, 0.09375, ((0, 2), (1, 32), (2, 8))),
        "shared_up": bell_draw(key_of[3], (LAYERS, D, FS), D ** -0.5, 0.09375, ((0, 2), (1, 32), (2, 8))),
        "shared_down": bell_draw(key_of[4], (LAYERS, FS, D), FS ** -0.5, 0.1875, ((0, 2), (1, 8), (2, 32))),
        "expert_gate": bell_draw(key_of[5], (LAYERS, HELD, D, FE), D ** -0.5, 0.09375, ((0, 2), (1, 32), (3, 8))),
        "expert_up": bell_draw(key_of[6], (LAYERS, HELD, D, FE), D ** -0.5, 0.09375, ((0, 2), (1, 32), (3, 8))),
        "expert_down": bell_draw(key_of[7], (LAYERS, HELD, FE, D), FE ** -0.5, 0.1875, ((0, 2), (1, 32), (2, 8))),
        "expert_ids": draw_expert_ids(jax.random.fold_in(key_of[11], 71), 0),
        "expert_slots": draw_expert_slots(jax.random.fold_in(key_of[11], 71), 0),
        "route_weights": jnp.clip(jnp.exp(math.log(1.0) - 2.3025851 * jax.random.uniform(key_of[10], (LAYERS, MB, TOKENS, TOP), jnp.float32) ** steps_of(key_of[10], (LAYERS, MB, TOKENS, TOP), ((0, 2), (2, 32)), -0.2, 0.2)), 0.1, 1.0),
    }


def product(left, right):
    return jnp.dot(left, right, preferred_element_type=jnp.float32)

def apply_layer(state, gain, sh_gate, sh_up, sh_down, ex_gate, ex_up, ex_down, route_ids, slot_rank, weights):
    values = state.astype(jnp.float32)
    inverse_rms = lax.rsqrt(lax.optimization_barrier(jnp.mean(values * values, axis=-1, keepdims=True)) + 1e-06)
    normed = (values * inverse_rms * gain).astype(jnp.bfloat16)
    shared_hidden = (jax.nn.silu(product(normed, sh_gate)) * product(normed, sh_up)).astype(jnp.bfloat16)
    shared_out = product(shared_hidden, sh_down)
    valid = (route_ids < HELD) & (slot_rank >= 0)
    slot_code = jnp.where(valid, route_ids * CAP + slot_rank, -1).astype(jnp.int32)
    blocks = TOKENS // TE
    code_blocks = slot_code.reshape(blocks, TE, TOP)
    slot_range = jnp.arange(HELD * CAP, dtype=jnp.int32)
    picker = jnp.any(code_blocks[:, None, :, :] == slot_range[None, :, None, None], axis=3).astype(jnp.float32)
    buffers = jnp.einsum('bjt,btd->bjd', picker, normed.reshape(blocks, TE, D).astype(jnp.float32)).astype(jnp.bfloat16)
    expert_rows = buffers.reshape(blocks, HELD, CAP, D).transpose(1, 0, 2, 3).reshape(HELD, blocks * CAP, D)

    def one_expert(operands):
        rows, w_gate, w_up, w_down = operands
        hidden = (jax.nn.silu(product(rows, w_gate)) * product(rows, w_up)).astype(jnp.bfloat16)
        summed = jnp.zeros((rows.shape[0], D), jnp.float32)
        for group in range(N_TENSOR):
            part = product(hidden[:, group * FE_DEV:(group + 1) * FE_DEV], w_down[group * FE_DEV:(group + 1) * FE_DEV]).astype(jnp.bfloat16)
            part = lax.optimization_barrier(part)
            summed = summed + part.astype(jnp.float32)
        return summed
    outputs = lax.map(one_expert, (expert_rows, ex_gate, ex_up, ex_down))
    returned = outputs.reshape(HELD, blocks, CAP, D).transpose(1, 0, 2, 3).reshape(blocks, HELD * CAP, D)
    index = jnp.maximum(code_blocks, 0).reshape(blocks, TE * TOP)[:, :, None]
    picked = jnp.take_along_axis(returned, index, axis=1).reshape(TOKENS, TOP, D)
    route_share = jnp.where(slot_code >= 0, weights, jnp.float32(0.0))
    routed = lax.optimization_barrier(jnp.sum(route_share[:, :, None] * picked, axis=1))
    return (values + shared_out + routed).astype(jnp.bfloat16)

def reference(tokens, norm_gain, shared_gate, shared_up, shared_down, expert_gate, expert_up, expert_down, expert_ids, expert_slots, route_weights):
    states = []
    for layer_index in range(LAYERS):
        layer_out = []
        for batch_index in range(MB):
            if layer_index == 0:
                state = tokens[batch_index]
            else:
                state = states[layer_index - 1][batch_index]
            layer_out.append(apply_layer(state, norm_gain[layer_index], shared_gate[layer_index], shared_up[layer_index], shared_down[layer_index], expert_gate[layer_index], expert_up[layer_index], expert_down[layer_index], expert_ids[layer_index, batch_index], expert_slots[layer_index, batch_index], route_weights[layer_index, batch_index]))
        states.append(jnp.stack(layer_out))
    return jnp.stack(states)
```

```python
import functools

import jax
import jax.numpy as jnp
from jax import lax
from jax.experimental import pallas as pl
from jax.experimental.pallas import tpu as pltpu
from jax.sharding import Mesh, PartitionSpec as P

CAP = 3
HELD = 32
SUB = ("pipe", "x", "yh", "yl", "z")
SWAP = [(0, 1), (1, 0)]
F32 = jnp.float32
BF16 = jnp.bfloat16


def to_all(v, axis):
    return lax.all_to_all(v, axis, split_axis=0, concat_axis=0, tiled=True)


def copies_to_all(v, axis):
    return to_all(jnp.broadcast_to(v, (lax.axis_size(axis), *v.shape)), axis)


def swapped(v):
    return lax.ppermute(v, "pipe", SWAP)


def normed_part(g_ref, gain_ref, inv, t):
    return (g_ref[t].astype(F32) * inv * gain_ref[pl.ds(t, 1), :]).astype(BF16)


def inverse_rms(g_ref):
    parts, rows, width = g_ref.shape
    total = jnp.zeros((rows, 1), F32)
    for t in range(parts):
        v = g_ref[t].astype(F32)
        total += jnp.sum(v * v, axis=-1, keepdims=True)
    return lax.rsqrt(total / (parts * width) + 1e-6)


def gated(gate, up):
    return (gate / (1.0 + jnp.exp(-gate)) * up).astype(BF16)


def take(first, ours, theirs, into, sems):
    for at, pair in enumerate((ours, theirs)):
        @pl.when(first == 1 - at)
        def _(pair=pair):
            for i, (src, dst) in enumerate(zip(pair, into)):
                pltpu.make_async_copy(src, dst, sems.at[i]).start()


def expert_kernel(first, g_ref, gain_ref, og, ou, od, tg, tu, td, out_ref, wg, wu, wd, sems):
    parts, rows, width = g_ref.shape
    take(first[0], (og, ou, od), (tg, tu, td), (wg, wu, wd), sems)
    inv = inverse_rms(g_ref)
    gate = jnp.zeros((rows, wg.shape[1]), F32)
    up = jnp.zeros((rows, wg.shape[1]), F32)
    pltpu.make_async_copy(og, wg, sems.at[0]).wait()
    pltpu.make_async_copy(ou, wu, sems.at[1]).wait()
    for t in range(parts):
        n = normed_part(g_ref, gain_ref, inv, t)
        gate += jnp.dot(n, wg[t * width : (t + 1) * width], preferred_element_type=F32)
        up += jnp.dot(n, wu[t * width : (t + 1) * width], preferred_element_type=F32)
    hidden = gated(gate, up)
    pltpu.make_async_copy(od, wd, sems.at[2]).wait()
    for t in range(parts):
        out_ref[t] = jnp.dot(
            hidden, wd[:, t * width : (t + 1) * width], preferred_element_type=F32
        ).astype(BF16)


def shared_kernel(first, g_ref, gain_ref, ow, tw, out_ref, w, sems):
    parts, rows, width = g_ref.shape
    n_z, n_yl, block, _ = w.shape
    take(first[0], (ow,), (tw,), (w,), sems)
    inv = inverse_rms(g_ref)
    both = jnp.zeros((rows, 2 * block), F32)
    pltpu.make_async_copy(ow, w, sems.at[0]).wait()
    per = width // block
    for t in range(parts):
        n = normed_part(g_ref, gain_ref, inv, t)
        for i in range(per):
            j = t * per + i
            both += jnp.dot(
                n[:, i * block : (i + 1) * block],
                w[j % n_z, j // n_z, :, : 2 * block],
                preferred_element_type=F32,
            )
    hidden = gated(both[:, :block], both[:, block:])
    for t in range(parts):
        for i in range(per):
            j = t * per + i
            out_ref[t, :, i * block : (i + 1) * block] = jnp.dot(
                hidden, w[j % n_z, j // n_z, :, 2 * block :], preferred_element_type=F32
            ).astype(BF16)


def call(kernel, first, g, gain, weights, scratch, name):
    vmem = pl.BlockSpec(memory_space=pltpu.VMEM)
    held = pl.BlockSpec(memory_space=pl.ANY)
    rows = g.shape[1]
    return pl.pallas_call(
        kernel,
        out_shape=jax.ShapeDtypeStruct(g.shape, BF16),
        in_specs=[pl.BlockSpec(memory_space=pltpu.SMEM), vmem, vmem] + [held] * len(weights),
        out_specs=vmem,
        scratch_shapes=[pltpu.VMEM(s, BF16) for s in scratch]
        + [pltpu.SemaphoreType.DMA((len(scratch),))],
        compiler_params=pltpu.CompilerParams(vmem_limit_bytes=32 * 2**20),
        cost_estimate=pl.CostEstimate(
            flops=6 * rows * 4096 * 128, bytes_accessed=4 * 2**20, transcendentals=rows * 128
        ),
        name=name,
    )(first, g, gain, *weights)


def per_device(
    tokens, norm_gain, shared_gate, shared_up, shared_down, expert_gate, expert_up, expert_down,
    expert_ids, expert_slots, route_weights,
):
    pipe = lax.axis_index("pipe")
    lower = pipe == 0
    batches, block, width = tokens.shape
    total = batches * block
    half = total // 2
    codes_of = 10
    mine = 5
    slots = HELD * mine
    n_tensor = lax.axis_size("x") * lax.axis_size("yh")

    ids, ranks = expert_ids[0], expert_slots[0]
    batch = lax.broadcasted_iota(jnp.int32, ids.shape, 0)
    valid = (ids < HELD) & (ranks >= 0)
    code = jnp.where(valid, ids * codes_of + batch * CAP + ranks, -1)
    table = jnp.concatenate([code.astype(F32), route_weights[0]], axis=-1).reshape(total, -1)
    table_there = swapped(table)
    gain = norm_gain[0].reshape(n_tensor, width)
    gain_there = swapped(gain)

    share = jnp.concatenate([shared_gate[0], shared_up[0], shared_down[0]], axis=1)
    share = copies_to_all(share, "yl")
    share = lax.all_gather(share, "z", axis=0)
    share_there = swapped(share)

    own = (expert_gate[0, 0], expert_up[0, 0], expert_down[0, 0])
    there = tuple(swapped(w) for w in own)

    slot = lax.broadcasted_iota(jnp.int32, (slots, 1, 1), 0)
    target = slot // mine * codes_of + slot % mine + mine * pipe
    target_f = target.astype(F32)

    state = tokens.reshape(total, width)
    produced = []
    for layer in range(2):
        here = pipe == layer
        first = here.astype(jnp.int32).reshape(1)
        routes = jnp.where(here, table, table_there)
        layer_gain = jnp.where(here, gain, gain_there)
        top = routes.shape[1] // 2
        route_code, route_weight = routes[:, :top], routes[:, top:]
        match = target_f == route_code[None]
        picker = jnp.any(match, axis=-1).astype(BF16)
        combine = jnp.sum(jnp.where(match, route_weight[None], 0.0), axis=-1)

        sent = jnp.dot(picker, state, preferred_element_type=F32).astype(BF16)
        sent = sent.reshape(HELD, mine, width // 128, 128)
        sent = jnp.broadcast_to(sent, (2, *sent.shape)).reshape(2 * HELD, mine, width // 128, 128)
        came = to_all(sent, ("yh", "yl", "z")).reshape(2, slots, width)
        rows = copies_to_all(came, "x").reshape(n_tensor, slots, width)
        parts = call(
            expert_kernel, first, rows, layer_gain, (*own, *there),
            [w.shape for w in own], "expert",
        )
        parts = to_all(parts.reshape(-1, 2 * slots, width), "x")
        parts = parts.astype(F32).sum(axis=0).astype(BF16)
        parts = parts.reshape(2 * HELD, mine, width // 128, 128)
        back = to_all(parts, ("yh", "yl", "z")).reshape(2, slots, width)
        back = back.astype(F32).sum(axis=0)
        routed = lax.dot_general(
            combine, back, (((0,), (0,)), ((), ())), preferred_element_type=F32
        )

        ours = jnp.where(lower, state[:half], state[half:])
        pair = copies_to_all(ours, "yh")
        full = copies_to_all(pair, "x").reshape(n_tensor, half, width)
        terms = call(
            shared_kernel, first, full, layer_gain, (share, share_there), [share.shape], "shared"
        )
        terms = to_all(terms.reshape(-1, 2 * half, width), "x")
        terms = terms.astype(F32).sum(axis=0).astype(BF16).reshape(2, half, width)
        terms = to_all(terms, "yh").astype(F32).sum(axis=0)
        none = jnp.zeros_like(terms)
        placed = jnp.concatenate(
            [jnp.where(lower, terms, none), jnp.where(lower, none, terms)], axis=0
        )
        added = (routed + placed).astype(BF16)
        added_there = swapped(added)
        state = (state.astype(F32) + (added.astype(F32) + added_there.astype(F32))).astype(BF16)
        produced.append(state)
    out = jnp.where(lower, produced[0], produced[1])
    return out.reshape(1, batches, block, width)


def solution(mesh):
    fine = Mesh(mesh.devices.reshape(2, 4, 2, 4, 8), SUB)
    tensor, expert = ("x", "yh"), ("yl", "z")
    in_specs = (
        P(None, expert, tensor),
        P("pipe", None),
        P("pipe", expert, tensor),
        P("pipe", expert, tensor),
        P("pipe", tensor, expert),
        P("pipe", expert, None, tensor),
        P("pipe", expert, None, tensor),
        P("pipe", expert, tensor, None),
        P("pipe", None, expert, None),
        P("pipe", None, expert, None),
        P("pipe", None, expert, None),
    )
    return jax.shard_map(
        per_device, mesh=fine, in_specs=in_specs, out_specs=P("pipe", None, expert, tensor),
        check_vma=False,
    )
```
